32 devices in a mesh: grp: 2 (over x), sub: 16 (over z, y, core).
Axes of the slice: x: 2, y: 2, z: 4, core: 2. Of those that a mesh axis runs over, the one named last changes fastest.
Arguments:
- counts: int32 [32], P(('grp', 'sub')), may hold values from 1 to 3, as said below
- block_map: int32 [96], P(('grp', 'sub')), may hold values from 0 to 31
- perms: int32 [96, 256], P(('grp', 'sub')), may hold values from 0 to 255, each once within a row
- mass_ii: bfloat16 [96, 1024, 1024], P(('grp', 'sub')), may hold values from -0.005859375 to 0.005859375
- mass_ib: bfloat16 [96, 1024, 256], P(('grp', 'sub')), may hold values from -0.1875 to 0.1875
- mass_bb: bfloat16 [96, 256, 256], P(('grp', 'sub')), may hold values from -6 to 6
- constraint_modes: bfloat16 [96, 1024, 256], P(('grp', 'sub')), may hold values from -6 to 6
- fixed_modes: bfloat16 [96, 1024, 128], P(('grp', 'sub')), may hold values from -6 to 6
Outputs:
- blocks: float32 [32, 256, 256], P('grp', 'sub')
- coupling: float32 [96, 128, 256], P(('grp', 'sub'))
The draws below stay inside these ranges and needn't reach their ends.
Inputs may be any that keep to these rules, and one draw needn't show every extreme that they name: `counts`: at least one device uses all 3 slots and one uses a single slot.
All inputs are finite; a program needn't handle non-finite values.
Results may differ from the reference program's by a relative error of at most 0.0021.
Values sent between devices are 32-bit elements; how exact they have to be, the bound alone decides.
A program may use at most 128 MiB of HBM per device.

```python
import jax
import jax.numpy as jnp
from jax import lax

I = 1024
B = 256
K = 128
SLOTS = 3
NBG = 16
CAP = 96
N_GRP = 2
N_SUB = 16
DEVICES = 32


def draw_counts(key, part):
    raw = jax.random.randint(key, (DEVICES,), 0, 6)
    values = jnp.where(raw < 4, 1, jnp.where(raw == 4, 2, SLOTS))
    values = jnp.minimum(values, SLOTS)
    values = values.at[0].set(SLOTS).at[1].set(1)
    return values.astype(jnp.int32)


def place_ends(drawn, own_key, low, high):
    extent = drawn.shape
    place = [jax.random.randint(jax.random.fold_in(own_key, axis), (), 0, extent[axis]) for axis in range(len(extent))]
    drawn = drawn.at[tuple(place)].set(low)
    longest = extent.index(max(extent))
    place[longest] = (place[longest] + 1) % extent[longest]
    return drawn.at[tuple(place)].set(high)


def shard_levels(stream_key, shape, cuts, low, high):
    level, own = 1.0, jax.random.fold_in(stream_key, 6)
    for axis_at, parts in cuts:
        heights = jnp.exp(jax.random.uniform(jax.random.fold_in(own, axis_at), (parts,), jnp.float32, low / len(cuts), high / len(cuts)))
        level = level * jnp.repeat(heights, shape[axis_at] // parts).reshape([-1 if axis == axis_at else 1 for axis in range(len(shape))])
    return level


def scatter_about(key, extent, deviation, bound, shards=(), held_as=jnp.bfloat16):
    drawn = jax.random.normal(key, extent, jnp.float32) * deviation
    if len(shards) > 0:
        drawn = shard_levels(key, extent, shards, -0.22, 0.18) * drawn
    return jnp.clip(drawn, min=-bound, max=bound).astype(held_as)


def setup_inputs(seed: int = 0) -> dict:
    keys = jax.random.split(jax.random.key(seed), 9)
    return {
        "counts": draw_counts(jax.random.fold_in(keys[8], 71), 0),
        "block_map": place_ends(jax.random.randint(keys[1], (CAP,), 0, 2 * NBG), jax.random.fold_in(keys[1], 1), 0, (2 * NBG) - 1).astype(jnp.int32),
        "perms": jax.vmap(lambda own: jax.random.permutation(own, B))(jax.random.split(keys[2], CAP)).reshape((CAP, B)).astype(jnp.int32),
        "mass_ii": scatter_about(keys[3], (CAP, I, I), (I * I) ** -0.5, 0.005859375, ((0, 32),)),
        "mass_ib": scatter_about(keys[4], (CAP, I, B), I ** -0.5, 0.1875, ((0, 32),)),
        "mass_bb": scatter_about(keys[5], (CAP, B, B), 1.0, 6.0, ((0, 32),)),
        "constraint_modes": scatter_about(keys[6], (CAP, I, B), 1.0, 6.0, ((0, 32),)),
        "fixed_modes": scatter_about(keys[7], (CAP, I, K), 1.0, 6.0, ((0, 32),)),
    }


def contract(left, right):
    return lax.dot_general(left, right, (((0,), (0,)), ((), ())), preferred_element_type=jnp.float32)


def reduce_slot(mass_ii, mass_ib, mass_bb, constraint_modes, fixed_modes):
    product = jnp.dot(mass_ii, constraint_modes, preferred_element_type=jnp.float32).astype(jnp.bfloat16)
    cross = contract(constraint_modes, mass_ib)
    reduced = contract(constraint_modes, product) + cross + cross.T + mass_bb.astype(jnp.float32)
    coupled = contract(fixed_modes, product) + contract(fixed_modes, mass_ib)
    return reduced, coupled


def reference(counts, block_map, perms, mass_ii, mass_ib, mass_bb, constraint_modes, fixed_modes):
    width = mass_bb.shape[1]
    total_slots = mass_ii.shape[0]
    modes = fixed_modes.shape[2]

    def step(carry_blocks, items):
        slot_id, code, perm_row, m_ii, m_ib, m_bb, psi_slot, phi_slot = items
        device = slot_id // SLOTS
        used_flag = (slot_id % SLOTS) < counts[device]
        group_index = device // N_SUB

        def active_branch(unused):
            return reduce_slot(m_ii, m_ib, m_bb, psi_slot, phi_slot)

        def empty_branch(unused):
            return (jnp.zeros((width, width), jnp.float32), jnp.zeros((modes, width), jnp.float32))

        reduced, coupled = lax.cond(used_flag, active_branch, empty_branch, 0)
        target = ((group_index + code // NBG) % N_GRP) * NBG + code % NBG
        inverse = jnp.zeros((width,), jnp.int32).at[perm_row].set(jnp.arange(width, dtype=jnp.int32))
        placed = reduced[inverse][:, inverse]
        carry_blocks = carry_blocks.at[target.astype(jnp.int32)].add(placed)
        return carry_blocks, coupled

    start = jnp.zeros((NBG * N_GRP, width, width), jnp.float32)
    items = (jnp.arange(total_slots, dtype=jnp.int32), block_map, perms, mass_ii, mass_ib, mass_bb, constraint_modes, fixed_modes)
    blocks, coupling = lax.scan(step, start, items)
    return blocks, coupling
```

```python
import functools

import jax
import jax.numpy as jnp
from jax import lax
from jax.experimental import pallas as pl
from jax.experimental.pallas import tpu as pltpu
from jax.sharding import PartitionSpec as P

NBG = 16
ROWS = 8
MESH = pl.DeviceIdType.MESH


def split(value):
    high = value.astype(jnp.bfloat16)
    low = (value - high.astype(jnp.float32)).astype(jnp.bfloat16)
    return high, low


def dot(left, right, left_dim=1, right_dim=0):
    return lax.dot_general(
        left,
        right,
        (((left_dim,), (right_dim,)), ((), ())),
        preferred_element_type=jnp.float32,
    )


def send_order(peers):
    return sorted(range(1, peers), key=lambda step: (abs(step - peers // 2), step))


def kernel(
    n_grp,
    n_sub,
    counts,
    codes,
    perms,
    mass_ii,
    mass_ib,
    mass_bb,
    psi_in,
    phi_in,
    blocks,
    coupling,
    m_ii,
    m_ib,
    m_bb,
    psi,
    phi,
    product,
    placed,
    got,
    key_mine,
    key_got,
    hot,
    home,
    ahead,
    passed,
    in_sem,
    send_sem,
    got_sem,
    key_send_sem,
    key_sem,
    pass_send_sem,
    pass_sem,
):
    grp = lax.axis_index("grp")
    me = lax.axis_index("sub")
    slots, interior, width = psi.shape
    chunks = got.shape[0]
    own_rows = chunks * ROWS
    lanes = n_sub * ROWS
    after = lax.rem(grp + 1, n_grp)
    before = lax.rem(grp + n_grp - 1, n_grp)

    def loads(slot):
        pairs = ((psi_in, psi), (mass_ii, m_ii), (mass_ib, m_ib), (mass_bb, m_bb), (phi_in, phi))
        return [
            pltpu.make_async_copy(source.at[slot], held.at[slot], in_sem.at[slot, index])
            for index, (source, held) in enumerate(pairs)
        ]

    for copy in loads(0):
        copy.start()

    order = send_order(n_sub)
    peers = [lax.rem(me + step, n_sub) for step in order]
    barrier = pltpu.get_barrier_semaphore()
    for peer in peers:
        pl.semaphore_signal(barrier, inc=1, device_id=(grp, peer), device_id_type=MESH)
    pl.semaphore_signal(barrier, inc=1, device_id=(after, me), device_id_type=MESH)
    greeted = len(peers) + 1
    if n_grp > 2:
        pl.semaphore_signal(barrier, inc=1, device_id=(before, me), device_id_type=MESH)
        greeted += 1

    lane = lax.broadcasted_iota(jnp.int32, (1, lanes), 1)
    key_mine[...] = jnp.zeros_like(key_mine)
    for slot in range(slots):
        code = jnp.where(slot < counts[0], codes[slot] * ROWS, -2 * NBG * ROWS)
        key_mine[slot : slot + 1, :] = jnp.where(lane // ROWS == me, code + lane % ROWS, 0)
    key_got[pl.ds(me, 1)] = key_mine[...][None]

    def key_copy(peer):
        return pltpu.make_async_remote_copy(
            src_ref=key_mine,
            dst_ref=key_got.at[me],
            send_sem=key_send_sem,
            recv_sem=key_sem,
            device_id=(grp, peer),
            device_id_type=MESH,
        )

    @pl.loop(0, slots)
    def one_slot(slot):
        copies = loads(slot)

        @pl.when(slot + 1 < slots)
        def ahead_loads():
            for copy in loads(slot + 1):
                copy.start()

        copies[0].wait()
        copies[1].wait()
        modes = psi[slot]
        step = min(interior, 256)
        for top in range(0, interior, step):
            product[top : top + step, :] = dot(m_ii[slot, top : top + step, :], modes).astype(
                jnp.bfloat16
            )
        for copy in copies[2:]:
            copy.wait()
        mixed = m_ib[slot]
        made = product[...]
        reduced = dot(modes, made, 0, 0) + dot(modes, mixed, 0, 0) + dot(mixed, modes, 0, 0)
        reduced = reduced + m_bb[slot].astype(jnp.float32)
        place = lax.broadcasted_iota(jnp.int32, (width, width), 0)
        pick = jnp.where(place == perms[pl.ds(slot, 1), :], 1.0, 0.0).astype(jnp.bfloat16)
        high, low = split(reduced)
        high = dot(high, pick, 1, 1).astype(jnp.bfloat16)
        low = dot(low, pick, 1, 1).astype(jnp.bfloat16)
        placed[slot] = dot(pick, high) + dot(pick, low)
        active = jnp.where(slot < counts[0], 1.0, 0.0)
        fixed = phi[slot]
        coupling[slot] = (dot(fixed, made, 0, 0) + dot(fixed, mixed, 0, 0)) * active
        for chunk in range(chunks):
            mine = pl.multiple_of(me * own_rows + chunk * ROWS, ROWS)
            got[chunk, slot, pl.ds(me, 1)] = placed[slot, pl.ds(mine, ROWS), :][None]

        @pl.when(slot == 0)
        def enter():
            pl.semaphore_wait(barrier, greeted)
            for peer in peers:
                key_copy(peer).start()

        for chunk in range(chunks):
            for peer in peers:
                top = pl.multiple_of(peer * own_rows + chunk * ROWS, ROWS)
                pltpu.make_async_remote_copy(
                    src_ref=placed.at[slot, pl.ds(top, ROWS), :],
                    dst_ref=got.at[chunk, slot, me],
                    send_sem=send_sem.at[chunk, slot],
                    recv_sem=got_sem.at[chunk, slot],
                    device_id=(grp, peer),
                    device_id_type=MESH,
                ).start()

    many = n_sub - 1
    all_keys = key_got.at[pl.ds(0, many)]
    pltpu.make_async_copy(all_keys, all_keys, key_sem).wait()
    keys = jnp.sum(key_got[...], axis=0)
    target = lax.broadcasted_iota(jnp.int32, (2 * NBG * ROWS, lanes), 0)
    for slot in range(slots):
        hot[slot] = jnp.where(target == keys[slot : slot + 1, :], 1.0, 0.0).astype(jnp.bfloat16)

    def pass_copy(chunk):
        return pltpu.make_async_remote_copy(
            src_ref=ahead.at[chunk],
            dst_ref=passed.at[chunk],
            send_sem=pass_send_sem.at[chunk],
            recv_sem=pass_sem.at[chunk],
            device_id=(after, me),
            device_id_type=MESH,
        )

    for chunk in range(chunks):
        total = None
        for slot in range(slots):
            arrived = got.at[chunk, slot, pl.ds(0, many)]
            pltpu.make_async_copy(arrived, arrived, got_sem.at[chunk, slot]).wait()
            high, low = split(got[chunk, slot].reshape(lanes, width))
            part = dot(hot[slot], high) + dot(hot[slot], low)
            total = part if total is None else total + part
        ahead[chunk] = total[NBG * ROWS :]
        home[chunk] = total[: NBG * ROWS]
        pass_copy(chunk).start()

    for chunk in range(chunks):
        pass_copy(chunk).wait()
        own = home[chunk] + passed[chunk]
        blocks[:, chunk * ROWS : (chunk + 1) * ROWS, :] = own.reshape(NBG, ROWS, width)

    pltpu.make_async_copy(all_keys, all_keys, key_send_sem).wait()
    for chunk in range(chunks):
        for slot in range(slots):
            arrived = got.at[chunk, slot, pl.ds(0, many)]
            pltpu.make_async_copy(arrived, arrived, send_sem.at[chunk, slot]).wait()


def per_device(n_grp, n_sub, counts, block_map, perms, mass_ii, mass_ib, mass_bb, psi, phi):
    slots, interior, width = psi.shape
    modes = phi.shape[2]
    own_rows = width // n_sub
    chunks = own_rows // ROWS
    lanes = n_sub * ROWS
    key_rows = -(-slots // 8) * 8
    smem = pl.BlockSpec(memory_space=pltpu.SMEM)
    vmem = pl.BlockSpec(memory_space=pltpu.VMEM)
    hbm = pl.BlockSpec(memory_space=pl.ANY)
    bf16, f32, i32 = jnp.bfloat16, jnp.float32, jnp.int32
    dma = pltpu.SemaphoreType.DMA
    return pl.pallas_call(
        functools.partial(kernel, n_grp, n_sub),
        out_shape=(
            jax.ShapeDtypeStruct((NBG, own_rows, width), f32),
            jax.ShapeDtypeStruct((slots, modes, width), f32),
        ),
        in_specs=[smem, smem, vmem] + [hbm] * 5,
        out_specs=(vmem, vmem),
        scratch_shapes=[
            pltpu.VMEM(mass_ii.shape, bf16),
            pltpu.VMEM(mass_ib.shape, bf16),
            pltpu.VMEM(mass_bb.shape, bf16),
            pltpu.VMEM(psi.shape, bf16),
            pltpu.VMEM(phi.shape, bf16),
            pltpu.VMEM((interior, width), bf16),
            pltpu.VMEM((slots, width, width), f32),
            pltpu.VMEM((chunks, slots, n_sub, ROWS, width), f32),
            pltpu.VMEM((key_rows, lanes), i32),
            pltpu.VMEM((n_sub, key_rows, lanes), i32),
            pltpu.VMEM((slots, 2 * NBG * ROWS, lanes), bf16),
            pltpu.VMEM((chunks, NBG * ROWS, width), f32),
            pltpu.VMEM((chunks, NBG * ROWS, width), f32),
            pltpu.VMEM((chunks, NBG * ROWS, width), f32),
            dma((slots, 5)),
            dma((chunks, slots)),
            dma((chunks, slots)),
            dma,
            dma,
            dma((chunks,)),
            dma((chunks,)),
        ],
        compiler_params=pltpu.CompilerParams(
            collective_id=0, has_side_effects=True, vmem_limit_bytes=56 * 1024 * 1024
        ),
    )(counts, block_map, perms, mass_ii, mass_ib, mass_bb, psi, phi)


def solution(mesh):
    both = P(("grp", "sub"))
    return jax.shard_map(
        functools.partial(per_device, mesh.shape["grp"], mesh.shape["sub"]),
        mesh=mesh,
        in_specs=(both,) * 8,
        out_specs=(P("grp", "sub", None), both),
        check_vma=False,
    )
```

```python
import functools

import jax
import jax.numpy as jnp
from jax import lax
from jax.experimental import pallas as pl
from jax.experimental.pallas import tpu as pltpu
from jax.sharding import PartitionSpec as P

NBG = 16
ROWS = 8
LANES = 128
WINDOW = 2
MESH = pl.DeviceIdType.MESH


def split(value):
    high = value.astype(jnp.bfloat16)
    low = (value - high.astype(jnp.float32)).astype(jnp.bfloat16)
    return high, low


def dot(left, right, left_dim=1, right_dim=0):
    return lax.dot_general(
        left,
        right,
        (((left_dim,), (right_dim,)), ((), ())),
        preferred_element_type=jnp.float32,
    )


def send_order(peers):
    return sorted(range(1, peers), key=lambda step: (abs(step - peers // 2), step))


def kernel(
    n_grp,
    n_sub,
    counts,
    codes,
    perms,
    mass_ii,
    mass_ib,
    mass_bb,
    psi_in,
    phi_in,
    blocks,
    coupling,
    m_ii,
    m_ib,
    m_bb,
    psi,
    phi,
    product,
    placed,
    got,
    key_mine,
    key_got,
    hot,
    sums,
    passed,
    in_sem,
    send_sem,
    got_sem,
    key_send_sem,
    key_sem,
    pass_send_sem,
    pass_sem,
):
    grp = lax.axis_index("grp")
    me = lax.axis_index("sub")
    slots, interior, width = psi.shape
    chunks = got.shape[0]
    cuts = width // LANES
    own_rows = chunks // cuts * ROWS
    lanes = n_sub * ROWS
    after = lax.rem(grp + 1, n_grp)
    before = lax.rem(grp + n_grp - 1, n_grp)

    def loads(slot):
        pairs = ((psi_in, psi), (mass_ii, m_ii), (mass_ib, m_ib), (mass_bb, m_bb), (phi_in, phi))
        return [
            pltpu.make_async_copy(source.at[slot], held.at[slot], in_sem.at[slot, index])
            for index, (source, held) in enumerate(pairs)
        ]

    for copy in loads(0):
        copy.start()

    order = send_order(n_sub)
    peers = [lax.rem(me + step, n_sub) for step in order]
    barrier = pltpu.get_barrier_semaphore()
    for peer in peers:
        pl.semaphore_signal(barrier, inc=1, device_id=(grp, peer), device_id_type=MESH)
    pl.semaphore_signal(barrier, inc=1, device_id=(after, me), device_id_type=MESH)
    greeted = len(peers) + 1
    if n_grp > 2:
        pl.semaphore_signal(barrier, inc=1, device_id=(before, me), device_id_type=MESH)
        greeted += 1

    lane = lax.broadcasted_iota(jnp.int32, (1, lanes), 1)
    key_mine[...] = jnp.zeros_like(key_mine)
    for slot in range(slots):
        code = jnp.where(slot < counts[0], codes[slot] * ROWS, -2 * NBG * ROWS)
        key_mine[slot : slot + 1, :] = jnp.where(lane // ROWS == me, code + lane % ROWS, 0)
    key_got[pl.ds(me, 1)] = key_mine[...][None]

    def key_copy(peer):
        return pltpu.make_async_remote_copy(
            src_ref=key_mine,
            dst_ref=key_got.at[me],
            send_sem=key_send_sem,
            recv_sem=key_sem,
            device_id=(grp, peer),
            device_id_type=MESH,
        )

    def send(chunk, slot):
        for peer in peers:
            top = pl.multiple_of(peer * own_rows + chunk // cuts * ROWS, ROWS)
            left = chunk % cuts * LANES
            pltpu.make_async_remote_copy(
                src_ref=placed.at[slot, pl.ds(top, ROWS), pl.ds(left, LANES)],
                dst_ref=got.at[chunk, slot, me],
                send_sem=send_sem.at[chunk, slot],
                recv_sem=got_sem.at[chunk, slot],
                device_id=(grp, peer),
                device_id_type=MESH,
            ).start()

    @pl.loop(0, slots)
    def one_slot(slot):
        copies = loads(slot)

        @pl.when(slot + 1 < slots)
        def ahead_loads():
            for copy in loads(slot + 1):
                copy.start()

        copies[0].wait()
        copies[1].wait()
        modes = psi[slot]
        step = min(interior, 256)
        for top in range(0, interior, step):
            product[top : top + step, :] = dot(m_ii[slot, top : top + step, :], modes).astype(
                jnp.bfloat16
            )
        for copy in copies[2:]:
            copy.wait()
        mixed = m_ib[slot]
        made = product[...]
        reduced = dot(modes, made, 0, 0) + dot(modes, mixed, 0, 0) + dot(mixed, modes, 0, 0)
        reduced = reduced + m_bb[slot].astype(jnp.float32)
        place = lax.broadcasted_iota(jnp.int32, (width, width), 0)
        pick = jnp.where(place == perms[pl.ds(slot, 1), :], 1.0, 0.0).astype(jnp.bfloat16)
        high, low = split(reduced)
        high = dot(high, pick, 1, 1).astype(jnp.bfloat16)
        low = dot(low, pick, 1, 1).astype(jnp.bfloat16)
        placed[slot] = dot(pick, high) + dot(pick, low)
        active = jnp.where(slot < counts[0], 1.0, 0.0)
        fixed = phi[slot]
        coupling[slot] = (dot(fixed, made, 0, 0) + dot(fixed, mixed, 0, 0)) * active
        for chunk in range(chunks):
            mine = pl.multiple_of(me * own_rows + chunk // cuts * ROWS, ROWS)
            left = chunk % cuts * LANES
            own = placed[slot, pl.ds(mine, ROWS), left : left + LANES]
            got[chunk, slot, pl.ds(me, 1)] = own[None]

        @pl.when(slot == 0)
        def enter():
            pl.semaphore_wait(barrier, greeted)
            for peer in peers:
                key_copy(peer).start()

        @pl.when(slot < slots - 1)
        def spread():
            for chunk in range(chunks):
                send(chunk, slot)

    window = min(WINDOW, chunks)
    for chunk in range(window):
        send(chunk, slots - 1)

    many = n_sub - 1
    all_keys = key_got.at[pl.ds(0, many)]
    pltpu.make_async_copy(all_keys, all_keys, key_sem).wait()
    keys = jnp.sum(key_got[...], axis=0)
    target = lax.broadcasted_iota(jnp.int32, (2 * NBG * ROWS, lanes), 0)
    for slot in range(slots):
        hot[slot] = jnp.where(target == keys[slot : slot + 1, :], 1.0, 0.0).astype(jnp.bfloat16)

    def pass_copy(chunk):
        return pltpu.make_async_remote_copy(
            src_ref=sums.at[chunk, pl.ds(NBG * ROWS, NBG * ROWS)],
            dst_ref=passed.at[chunk],
            send_sem=pass_send_sem.at[chunk],
            recv_sem=pass_sem.at[chunk],
            device_id=(after, me),
            device_id_type=MESH,
        )

    def owner_sum(chunk, slot):
        arrived = got.at[chunk, slot, pl.ds(0, many)]
        pltpu.make_async_copy(arrived, arrived, got_sem.at[chunk, slot]).wait()
        high, low = split(got[chunk, slot].reshape(lanes, LANES))
        return dot(hot[slot], high) + dot(hot[slot], low)

    for slot in range(slots):
        for chunk in range(chunks):
            total = owner_sum(chunk, slot)
            if slot > 0:
                total = total + sums[chunk]
            sums[chunk] = total
            if slot == slots - 1:
                pass_copy(chunk).start()
                if chunk + window < chunks:
                    send(chunk + window, slot)

    for chunk in range(chunks):
        pass_copy(chunk).wait()
        own = sums[chunk, : NBG * ROWS] + passed[chunk]
        top, left = chunk // cuts * ROWS, chunk % cuts * LANES
        blocks[:, top : top + ROWS, left : left + LANES] = own.reshape(NBG, ROWS, LANES)

    pltpu.make_async_copy(all_keys, all_keys, key_send_sem).wait()
    for chunk in range(chunks):
        for slot in range(slots):
            arrived = got.at[chunk, slot, pl.ds(0, many)]
            pltpu.make_async_copy(arrived, arrived, send_sem.at[chunk, slot]).wait()


def halves_kernel(
    n_grp,
    n_sub,
    counts,
    codes,
    perms,
    mass_ii,
    mass_ib,
    mass_bb,
    psi_in,
    phi_in,
    blocks,
    coupling,
    m_ii,
    m_ib,
    m_bb,
    psi,
    phi,
    product,
    placed,
    got,
    key_mine,
    key_got,
    hot,
    sums,
    passed,
    in_sem,
    send_sem,
    got_sem,
    key_send_sem,
    key_sem,
    pass_send_sem,
    pass_sem,
):
    grp = lax.axis_index("grp")
    me = lax.axis_index("sub")
    slots, interior, width = psi.shape
    own_rows = width // n_sub
    half = n_sub // 2
    lanes = n_sub * ROWS
    part_rows = NBG * ROWS
    other = 1 - grp
    far = lax.rem(me + half, n_sub)
    member = grp * half + lax.rem(me, half)
    first = me - lax.rem(me, half)

    def loads(slot):
        pairs = ((psi_in, psi), (mass_ii, m_ii), (mass_ib, m_ib), (mass_bb, m_bb), (phi_in, phi))
        return [
            pltpu.make_async_copy(source.at[slot], held.at[slot], in_sem.at[slot, index])
            for index, (source, held) in enumerate(pairs)
        ]

    for copy in loads(0):
        copy.start()

    peers = []
    for step in send_order(n_sub):
        index = lax.rem(member + step, n_sub)
        peers.append((index // half, first + lax.rem(index, half)))
    barrier = pltpu.get_barrier_semaphore()
    for peer in peers + [(grp, far), (other, far)]:
        pl.semaphore_signal(barrier, inc=1, device_id=peer, device_id_type=MESH)
    greeted = len(peers) + 2

    lane = lax.broadcasted_iota(jnp.int32, (1, lanes), 1)
    key_mine[...] = jnp.zeros_like(key_mine)
    for slot in range(slots):
        code = codes[slot]
        block = lax.rem(grp + code // NBG, n_grp) * NBG + lax.rem(code, NBG)
        block = jnp.where(slot < counts[0], block, -n_grp * NBG) * ROWS
        key_mine[slot : slot + 1, :] = jnp.where(lane // ROWS == member, block + lane % ROWS, 0)
    key_got[pl.ds(member, 1)] = key_mine[...][None]

    def key_copy(peer):
        return pltpu.make_async_remote_copy(
            src_ref=key_mine,
            dst_ref=key_got.at[member],
            send_sem=key_send_sem,
            recv_sem=key_sem,
            device_id=peer,
            device_id_type=MESH,
        )

    def row_of(part, peer):
        owner = lax.rem(peer[1] + half, n_sub) if part == 0 else peer[1]
        return pl.multiple_of(owner * own_rows + peer[0] * ROWS, ROWS)

    def send(part, slot):
        for peer in peers:
            pltpu.make_async_remote_copy(
                src_ref=placed.at[slot, pl.ds(row_of(part, peer), ROWS), :],
                dst_ref=got.at[part, slot, member],
                send_sem=send_sem.at[part, slot],
                recv_sem=got_sem.at[part, slot],
                device_id=peer,
                device_id_type=MESH,
            ).start()

    @pl.loop(0, slots)
    def one_slot(slot):
        copies = loads(slot)

        @pl.when(slot + 1 < slots)
        def ahead_loads():
            for copy in loads(slot + 1):
                copy.start()

        copies[0].wait()
        copies[1].wait()
        modes = psi[slot]
        step = min(interior, 256)
        for top in range(0, interior, step):
            product[top : top + step, :] = dot(m_ii[slot, top : top + step, :], modes).astype(
                jnp.bfloat16
            )
        for copy in copies[2:]:
            copy.wait()
        mixed = m_ib[slot]
        made = product[...]
        reduced = dot(modes, made, 0, 0) + dot(modes, mixed, 0, 0) + dot(mixed, modes, 0, 0)
        reduced = reduced + m_bb[slot].astype(jnp.float32)
        place = lax.broadcasted_iota(jnp.int32, (width, width), 0)
        pick = jnp.where(place == perms[pl.ds(slot, 1), :], 1.0, 0.0).astype(jnp.bfloat16)
        high, low = split(reduced)
        high = dot(high, pick, 1, 1).astype(jnp.bfloat16)
        low = dot(low, pick, 1, 1).astype(jnp.bfloat16)
        placed[slot] = dot(pick, high) + dot(pick, low)
        active = jnp.where(slot < counts[0], 1.0, 0.0)
        fixed = phi[slot]
        coupling[slot] = (dot(fixed, made, 0, 0) + dot(fixed, mixed, 0, 0)) * active
        for part in range(2):
            own = placed[slot, pl.ds(row_of(part, (grp, me)), ROWS), :]
            got[part, slot, pl.ds(member, 1)] = own[None]

        @pl.when(slot == 0)
        def enter():
            pl.semaphore_wait(barrier, greeted)
            for peer in peers:
                key_copy(peer).start()

        send(0, slot)

    for slot in range(slots):
        send(1, slot)

    many = n_sub - 1
    all_keys = key_got.at[pl.ds(0, many)]
    pltpu.make_async_copy(all_keys, all_keys, key_sem).wait()
    keys = jnp.sum(key_got[...], axis=0)
    target = lax.broadcasted_iota(jnp.int32, (2 * NBG * ROWS, lanes), 0)
    for slot in range(slots):
        hot[slot] = jnp.where(target == keys[slot : slot + 1, :], 1.0, 0.0).astype(jnp.bfloat16)

    def pass_copy(source, part, place, peer):
        return pltpu.make_async_remote_copy(
            src_ref=sums.at[source, pl.ds(pl.multiple_of(part * part_rows, part_rows), part_rows)],
            dst_ref=passed.at[place],
            send_sem=pass_send_sem.at[source],
            recv_sem=pass_sem.at[place],
            device_id=peer,
            device_id_type=MESH,
        )

    def owner_sum(part):
        total = None
        for slot in range(slots):
            arrived = got.at[part, slot, pl.ds(0, many)]
            pltpu.make_async_copy(arrived, arrived, got_sem.at[part, slot]).wait()
            high, low = split(got[part, slot].reshape(lanes, width))
            one = dot(hot[slot], high) + dot(hot[slot], low)
            total = one if total is None else total + one
        sums[part] = total

    owner_sum(0)
    pass_copy(0, other, grp, (other, far)).start()
    pass_copy(0, grp, grp, (grp, far)).start()
    owner_sum(1)
    pass_copy(1, other, 2, (other, me)).start()

    pltpu.make_async_copy(all_keys, all_keys, key_send_sem).wait()
    for part in range(2):
        for slot in range(slots):
            arrived = got.at[part, slot, pl.ds(0, many)]
            pltpu.make_async_copy(arrived, arrived, send_sem.at[part, slot]).wait()

    for place in range(3):
        pltpu.make_async_copy(passed.at[place], passed.at[place], pass_sem.at[place]).wait()
    kept = sums[1, pl.ds(pl.multiple_of(grp * part_rows, part_rows), part_rows), :]
    for row, near in ((grp, kept), (other, passed[2])):
        value = (passed[row] + near).reshape(NBG, ROWS, width)
        blocks[:, pl.ds(pl.multiple_of(row * ROWS, ROWS), ROWS), :] = value

    both = sums.at[0]
    pltpu.make_async_copy(both, both, pass_send_sem.at[0]).wait()
    pltpu.make_async_copy(passed.at[2], passed.at[2], pass_send_sem.at[1]).wait()


def per_device(n_grp, n_sub, counts, block_map, perms, mass_ii, mass_ib, mass_bb, psi, phi):
    slots, interior, width = psi.shape
    modes = phi.shape[2]
    own_rows = width // n_sub
    chunks = own_rows // ROWS * (width // LANES)
    cut = LANES
    lanes = n_sub * ROWS
    body = kernel
    places = chunks
    if n_grp == 2 and own_rows == 2 * ROWS and n_sub % 2 == 0:
        body, chunks, places, cut = halves_kernel, 2, 3, width
    key_rows = -(-slots // 8) * 8
    smem = pl.BlockSpec(memory_space=pltpu.SMEM)
    vmem = pl.BlockSpec(memory_space=pltpu.VMEM)
    hbm = pl.BlockSpec(memory_space=pl.ANY)
    bf16, f32, i32 = jnp.bfloat16, jnp.float32, jnp.int32
    dma = pltpu.SemaphoreType.DMA
    return pl.pallas_call(
        functools.partial(body, n_grp, n_sub),
        out_shape=(
            pltpu.VMEM((NBG, own_rows, width), f32),
            pltpu.VMEM((slots, modes, width), f32),
        ),
        in_specs=[smem, smem, vmem] + [hbm] * 5,
        out_specs=(vmem, vmem),
        scratch_shapes=[
            pltpu.VMEM(mass_ii.shape, bf16),
            pltpu.VMEM(mass_ib.shape, bf16),
            pltpu.VMEM(mass_bb.shape, bf16),
            pltpu.VMEM(psi.shape, bf16),
            pltpu.VMEM(phi.shape, bf16),
            pltpu.VMEM((interior, width), bf16),
            pltpu.VMEM((slots, width, width), f32),
            pltpu.VMEM((chunks, slots, n_sub, ROWS, cut), f32),
            pltpu.VMEM((key_rows, lanes), i32),
            pltpu.VMEM((n_sub, key_rows, lanes), i32),
            pltpu.VMEM((slots, 2 * NBG * ROWS, lanes), bf16),
            pltpu.VMEM((chunks, 2 * NBG * ROWS, cut), f32),
            pltpu.VMEM((places, NBG * ROWS, cut), f32),
            dma((slots, 5)),
            dma((chunks, slots)),
            dma((chunks, slots)),
            dma,
            dma,
            dma((chunks,)),
            dma((places,)),
        ],
        compiler_params=pltpu.CompilerParams(
            collective_id=0, has_side_effects=True, vmem_limit_bytes=56 * 1024 * 1024
        ),
    )(counts, block_map, perms, mass_ii, mass_ib, mass_bb, psi, phi)


def solution(mesh):
    both = P(("grp", "sub"))
    return jax.shard_map(
        functools.partial(per_device, mesh.shape["grp"], mesh.shape["sub"]),
        mesh=mesh,
        in_specs=(both,) * 8,
        out_specs=(P("grp", "sub", None), both),
        check_vma=False,
    )
```

```python
import functools

import jax
import jax.numpy as jnp
from jax import lax
from jax.experimental import pallas as pl
from jax.experimental.pallas import tpu as pltpu
from jax.sharding import PartitionSpec as P

NBG = 16
ROWS = 8
LANES = 128
WINDOW = 2
MESH = pl.DeviceIdType.MESH


def split(value):
    high = value.astype(jnp.bfloat16)
    low = (value - high.astype(jnp.float32)).astype(jnp.bfloat16)
    return high, low


def dot(left, right, left_dim=1, right_dim=0):
    return lax.dot_general(
        left,
        right,
        (((left_dim,), (right_dim,)), ((), ())),
        preferred_element_type=jnp.float32,
    )


def send_order(peers):
    return sorted(range(1, peers), key=lambda step: (abs(step - peers // 2), step))


def kernel(
    n_grp,
    n_sub,
    counts,
    codes,
    perms,
    mass_ii,
    mass_ib,
    mass_bb,
    psi_in,
    phi_in,
    blocks,
    coupling,
    m_ii,
    m_bb,
    lhs,
    rhs,
    placed,
    got,
    key_mine,
    key_got,
    hot,
    sums,
    passed,
    in_sem,
    send_sem,
    got_sem,
    key_send_sem,
    key_sem,
    pass_send_sem,
    pass_sem,
):
    grp = lax.axis_index("grp")
    me = lax.axis_index("sub")
    slots, interior, width = psi_in.shape
    chunks = got.shape[0]
    cuts = width // LANES
    own_rows = chunks // cuts * ROWS
    lanes = n_sub * ROWS
    after = lax.rem(grp + 1, n_grp)
    before = lax.rem(grp + n_grp - 1, n_grp)

    def loads(slot):
        pairs = (
            (psi_in, lhs.at[slot, :, pl.ds(0, width)]),
            (mass_ii, m_ii.at[slot]),
            (mass_ib, rhs.at[slot, :, pl.ds(width, width)]),
            (mass_bb, m_bb.at[slot]),
            (phi_in, lhs.at[slot, :, pl.ds(width, lhs.shape[2] - width)]),
        )
        return [
            pltpu.make_async_copy(source.at[slot], held, in_sem.at[slot, index])
            for index, (source, held) in enumerate(pairs)
        ]

    for copy in loads(0):
        copy.start()

    order = send_order(n_sub)
    peers = [lax.rem(me + step, n_sub) for step in order]
    barrier = pltpu.get_barrier_semaphore()
    for peer in peers:
        pl.semaphore_signal(barrier, inc=1, device_id=(grp, peer), device_id_type=MESH)
    pl.semaphore_signal(barrier, inc=1, device_id=(after, me), device_id_type=MESH)
    greeted = len(peers) + 1
    if n_grp > 2:
        pl.semaphore_signal(barrier, inc=1, device_id=(before, me), device_id_type=MESH)
        greeted += 1

    lane = lax.broadcasted_iota(jnp.int32, (1, lanes), 1)
    key_mine[...] = jnp.zeros_like(key_mine)
    for slot in range(slots):
        code = jnp.where(slot < counts[0], codes[slot] * ROWS, -2 * NBG * ROWS)
        key_mine[slot : slot + 1, :] = jnp.where(lane // ROWS == me, code + lane % ROWS, 0)
    key_got[pl.ds(me, 1)] = key_mine[...][None]

    def key_copy(peer):
        return pltpu.make_async_remote_copy(
            src_ref=key_mine,
            dst_ref=key_got.at[me],
            send_sem=key_send_sem,
            recv_sem=key_sem,
            device_id=(grp, peer),
            device_id_type=MESH,
        )

    def send(chunk, slot):
        for peer in peers:
            top = pl.multiple_of(peer * own_rows + chunk // cuts * ROWS, ROWS)
            left = chunk % cuts * LANES
            pltpu.make_async_remote_copy(
                src_ref=placed.at[slot, pl.ds(top, ROWS), pl.ds(left, LANES)],
                dst_ref=got.at[chunk, slot, me],
                send_sem=send_sem.at[chunk, slot],
                recv_sem=got_sem.at[chunk, slot],
                device_id=(grp, peer),
                device_id_type=MESH,
            ).start()

    @pl.loop(0, slots)
    def one_slot(slot):
        copies = loads(slot)

        @pl.when(slot + 1 < slots)
        def ahead_loads():
            for copy in loads(slot + 1):
                copy.start()

        copies[0].wait()
        copies[1].wait()
        step = min(interior, 256)
        modes = lhs[slot, :, :width]
        for top in range(0, interior, step):
            made = dot(m_ii[slot, top : top + step, :], modes).astype(jnp.bfloat16)
            rhs[slot, top : top + step, :width] = made
        for copy in copies[2:]:
            copy.wait()
        every = dot(lhs[slot], rhs[slot], 0, 0)
        cross = every[:width, width:]
        direct = every[:width, :width] + cross + m_bb[slot].astype(jnp.float32)
        place = lax.broadcasted_iota(jnp.int32, (width, width), 0)
        pick = jnp.where(place == perms[pl.ds(slot, 1), :], 1.0, 0.0).astype(jnp.bfloat16)
        high, low = split(direct)
        cross_high, cross_low = split(cross)
        rows = dot(pick, high) + dot(pick, low)
        rows = rows + dot(pick, cross_high, 1, 1) + dot(pick, cross_low, 1, 1)
        high, low = split(rows)
        placed[slot] = dot(high, pick, 1, 1) + dot(low, pick, 1, 1)
        active = jnp.where(slot < counts[0], 1.0, 0.0)
        coupling[slot] = (every[width:, :width] + every[width:, width:]) * active
        for chunk in range(chunks):
            mine = pl.multiple_of(me * own_rows + chunk // cuts * ROWS, ROWS)
            left = chunk % cuts * LANES
            own = placed[slot, pl.ds(mine, ROWS), left : left + LANES]
            got[chunk, slot, pl.ds(me, 1)] = own[None]

        @pl.when(slot == 0)
        def enter():
            pl.semaphore_wait(barrier, greeted)
            for peer in peers:
                key_copy(peer).start()

        @pl.when(slot < slots - 1)
        def spread():
            for chunk in range(chunks):
                send(chunk, slot)

    window = min(WINDOW, chunks)
    for chunk in range(window):
        send(chunk, slots - 1)

    many = n_sub - 1
    all_keys = key_got.at[pl.ds(0, many)]
    pltpu.make_async_copy(all_keys, all_keys, key_sem).wait()
    keys = jnp.sum(key_got[...], axis=0)
    target = lax.broadcasted_iota(jnp.int32, (2 * NBG * ROWS, lanes), 0)
    for slot in range(slots):
        hot[slot] = jnp.where(target == keys[slot : slot + 1, :], 1.0, 0.0).astype(jnp.bfloat16)

    def pass_copy(chunk):
        return pltpu.make_async_remote_copy(
            src_ref=sums.at[chunk, pl.ds(NBG * ROWS, NBG * ROWS)],
            dst_ref=passed.at[chunk],
            send_sem=pass_send_sem.at[chunk],
            recv_sem=pass_sem.at[chunk],
            device_id=(after, me),
            device_id_type=MESH,
        )

    def owner_sum(chunk, slot):
        arrived = got.at[chunk, slot, pl.ds(0, many)]
        pltpu.make_async_copy(arrived, arrived, got_sem.at[chunk, slot]).wait()
        high, low = split(got[chunk, slot].reshape(lanes, LANES))
        return dot(hot[slot], high) + dot(hot[slot], low)

    for slot in range(slots):
        for chunk in range(chunks):
            total = owner_sum(chunk, slot)
            if slot > 0:
                total = total + sums[chunk]
            sums[chunk] = total
            if slot == slots - 1:
                pass_copy(chunk).start()
                if chunk + window < chunks:
                    send(chunk + window, slot)

    for chunk in range(chunks):
        pass_copy(chunk).wait()
        own = sums[chunk, : NBG * ROWS] + passed[chunk]
        top, left = chunk // cuts * ROWS, chunk % cuts * LANES
        blocks[:, top : top + ROWS, left : left + LANES] = own.reshape(NBG, ROWS, LANES)

    pltpu.make_async_copy(all_keys, all_keys, key_send_sem).wait()
    for chunk in range(chunks):
        for slot in range(slots):
            arrived = got.at[chunk, slot, pl.ds(0, many)]
            pltpu.make_async_copy(arrived, arrived, send_sem.at[chunk, slot]).wait()


def halves_kernel(
    n_grp,
    n_sub,
    counts,
    codes,
    perms,
    mass_ii,
    mass_ib,
    mass_bb,
    psi_in,
    phi_in,
    blocks,
    coupling,
    m_ii,
    m_bb,
    lhs,
    rhs,
    placed,
    got,
    key_mine,
    key_got,
    hot,
    sums,
    passed,
    in_sem,
    send_sem,
    got_sem,
    key_send_sem,
    key_sem,
    pass_send_sem,
    pass_sem,
):
    grp = lax.axis_index("grp")
    me = lax.axis_index("sub")
    slots, interior, width = psi_in.shape
    own_rows = width // n_sub
    half = n_sub // 2
    lanes = n_sub * ROWS
    part_rows = NBG * ROWS
    other = 1 - grp
    far = lax.rem(me + half, n_sub)
    member = grp * half + lax.rem(me, half)
    first = me - lax.rem(me, half)

    def loads(slot):
        pairs = (
            (psi_in, lhs.at[slot, :, pl.ds(0, width)]),
            (mass_ii, m_ii.at[slot]),
            (mass_ib, rhs.at[slot, :, pl.ds(width, width)]),
            (mass_bb, m_bb.at[slot]),
            (phi_in, lhs.at[slot, :, pl.ds(width, lhs.shape[2] - width)]),
        )
        return [
            pltpu.make_async_copy(source.at[slot], held, in_sem.at[slot, index])
            for index, (source, held) in enumerate(pairs)
        ]

    for copy in loads(0):
        copy.start()

    peers = []
    for step in send_order(n_sub):
        index = lax.rem(member + step, n_sub)
        peers.append((index // half, first + lax.rem(index, half)))
    barrier = pltpu.get_barrier_semaphore()
    for peer in peers + [(grp, far), (other, far)]:
        pl.semaphore_signal(barrier, inc=1, device_id=peer, device_id_type=MESH)
    greeted = len(peers) + 2

    lane = lax.broadcasted_iota(jnp.int32, (1, lanes), 1)
    key_mine[...] = jnp.zeros_like(key_mine)
    for slot in range(slots):
        code = codes[slot]
        block = lax.rem(grp + code // NBG, n_grp) * NBG + lax.rem(code, NBG)
        block = jnp.where(slot < counts[0], block, -n_grp * NBG) * ROWS
        key_mine[slot : slot + 1, :] = jnp.where(lane // ROWS == member, block + lane % ROWS, 0)
    key_got[pl.ds(member, 1)] = key_mine[...][None]

    def key_copy(peer):
        return pltpu.make_async_remote_copy(
            src_ref=key_mine,
            dst_ref=key_got.at[member],
            send_sem=key_send_sem,
            recv_sem=key_sem,
            device_id=peer,
            device_id_type=MESH,
        )

    def row_of(part, peer):
        owner = lax.rem(peer[1] + half, n_sub) if part == 0 else peer[1]
        return pl.multiple_of(owner * own_rows + peer[0] * ROWS, ROWS)

    def send(part, slot):
        for peer in peers:
            pltpu.make_async_remote_copy(
                src_ref=placed.at[slot, pl.ds(row_of(part, peer), ROWS), :],
                dst_ref=got.at[part, slot, member],
                send_sem=send_sem.at[part, slot],
                recv_sem=got_sem.at[part, slot],
                device_id=peer,
                device_id_type=MESH,
            ).start()

    @pl.loop(0, slots)
    def one_slot(slot):
        copies = loads(slot)

        @pl.when(slot + 1 < slots)
        def ahead_loads():
            for copy in loads(slot + 1):
                copy.start()

        copies[0].wait()
        copies[1].wait()
        step = min(interior, 256)
        modes = lhs[slot, :, :width]
        for top in range(0, interior, step):
            made = dot(m_ii[slot, top : top + step, :], modes).astype(jnp.bfloat16)
            rhs[slot, top : top + step, :width] = made
        for copy in copies[2:]:
            copy.wait()
        every = dot(lhs[slot], rhs[slot], 0, 0)
        cross = every[:width, width:]
        direct = every[:width, :width] + cross + m_bb[slot].astype(jnp.float32)
        place = lax.broadcasted_iota(jnp.int32, (width, width), 0)
        pick = jnp.where(place == perms[pl.ds(slot, 1), :], 1.0, 0.0).astype(jnp.bfloat16)
        high, low = split(direct)
        cross_high, cross_low = split(cross)
        rows = dot(pick, high) + dot(pick, low)
        rows = rows + dot(pick, cross_high, 1, 1) + dot(pick, cross_low, 1, 1)
        high, low = split(rows)
        placed[slot] = dot(high, pick, 1, 1) + dot(low, pick, 1, 1)
        active = jnp.where(slot < counts[0], 1.0, 0.0)
        coupling[slot] = (every[width:, :width] + every[width:, width:]) * active
        for part in range(2):
            own = placed[slot, pl.ds(row_of(part, (grp, me)), ROWS), :]
            got[part, slot, pl.ds(member, 1)] = own[None]

        @pl.when(slot == 0)
        def enter():
            pl.semaphore_wait(barrier, greeted)
            for peer in peers:
                key_copy(peer).start()

        send(0, slot)

    for slot in range(slots):
        send(1, slot)

    many = n_sub - 1
    all_keys = key_got.at[pl.ds(0, many)]
    pltpu.make_async_copy(all_keys, all_keys, key_sem).wait()
    keys = jnp.sum(key_got[...], axis=0)
    target = lax.broadcasted_iota(jnp.int32, (2 * NBG * ROWS, lanes), 0)
    for slot in range(slots):
        hot[slot] = jnp.where(target == keys[slot : slot + 1, :], 1.0, 0.0).astype(jnp.bfloat16)

    def pass_copy(source, part, place, peer):
        return pltpu.make_async_remote_copy(
            src_ref=sums.at[source, pl.ds(pl.multiple_of(part * part_rows, part_rows), part_rows)],
            dst_ref=passed.at[place],
            send_sem=pass_send_sem.at[source],
            recv_sem=pass_sem.at[place],
            device_id=peer,
            device_id_type=MESH,
        )

    def owner_sum(part):
        total = None
        for slot in range(slots):
            arrived = got.at[part, slot, pl.ds(0, many)]
            pltpu.make_async_copy(arrived, arrived, got_sem.at[part, slot]).wait()
            high, low = split(got[part, slot].reshape(lanes, width))
            one = dot(hot[slot], high) + dot(hot[slot], low)
            total = one if total is None else total + one
        sums[part] = total

    owner_sum(0)
    pass_copy(0, other, grp, (other, far)).start()
    pass_copy(0, grp, grp, (grp, far)).start()
    owner_sum(1)
    pass_copy(1, other, 2, (other, me)).start()

    pltpu.make_async_copy(all_keys, all_keys, key_send_sem).wait()
    for part in range(2):
        for slot in range(slots):
            arrived = got.at[part, slot, pl.ds(0, many)]
            pltpu.make_async_copy(arrived, arrived, send_sem.at[part, slot]).wait()

    for place in range(3):
        pltpu.make_async_copy(passed.at[place], passed.at[place], pass_sem.at[place]).wait()
    kept = sums[1, pl.ds(pl.multiple_of(grp * part_rows, part_rows), part_rows), :]
    for row, near in ((grp, kept), (other, passed[2])):
        value = (passed[row] + near).reshape(NBG, ROWS, width)
        blocks[:, pl.ds(pl.multiple_of(row * ROWS, ROWS), ROWS), :] = value

    both = sums.at[0]
    pltpu.make_async_copy(both, both, pass_send_sem.at[0]).wait()
    pltpu.make_async_copy(passed.at[2], passed.at[2], pass_send_sem.at[1]).wait()


def per_device(n_grp, n_sub, counts, block_map, perms, mass_ii, mass_ib, mass_bb, psi, phi):
    slots, interior, width = psi.shape
    modes = phi.shape[2]
    own_rows = width // n_sub
    chunks = own_rows // ROWS * (width // LANES)
    cut = LANES
    lanes = n_sub * ROWS
    body = kernel
    places = chunks
    if n_grp == 2 and own_rows == 2 * ROWS and n_sub % 2 == 0:
        body, chunks, places, cut = halves_kernel, 2, 3, width
    key_rows = -(-slots // 8) * 8
    smem = pl.BlockSpec(memory_space=pltpu.SMEM)
    vmem = pl.BlockSpec(memory_space=pltpu.VMEM)
    hbm = pl.BlockSpec(memory_space=pl.ANY)
    bf16, f32, i32 = jnp.bfloat16, jnp.float32, jnp.int32
    dma = pltpu.SemaphoreType.DMA
    return pl.pallas_call(
        functools.partial(body, n_grp, n_sub),
        out_shape=(
            pltpu.VMEM((NBG, own_rows, width), f32),
            pltpu.VMEM((slots, modes, width), f32),
        ),
        in_specs=[smem, smem, vmem] + [hbm] * 5,
        out_specs=(vmem, vmem),
        scratch_shapes=[
            pltpu.VMEM(mass_ii.shape, bf16),
            pltpu.VMEM(mass_bb.shape, bf16),
            pltpu.VMEM((slots, interior, width + modes), bf16),
            pltpu.VMEM((slots, interior, 2 * width), bf16),
            pltpu.VMEM((slots, width, width), f32),
            pltpu.VMEM((chunks, slots, n_sub, ROWS, cut), f32),
            pltpu.VMEM((key_rows, lanes), i32),
            pltpu.VMEM((n_sub, key_rows, lanes), i32),
            pltpu.VMEM((slots, 2 * NBG * ROWS, lanes), bf16),
            pltpu.VMEM((chunks, 2 * NBG * ROWS, cut), f32),
            pltpu.VMEM((places, NBG * ROWS, cut), f32),
            dma((slots, 5)),
            dma((chunks, slots)),
            dma((chunks, slots)),
            dma,
            dma,
            dma((chunks,)),
            dma((places,)),
        ],
        compiler_params=pltpu.CompilerParams(
            collective_id=0, has_side_effects=True, vmem_limit_bytes=56 * 1024 * 1024
        ),
    )(counts, block_map, perms, mass_ii, mass_ib, mass_bb, psi, phi)


def solution(mesh):
    both = P(("grp", "sub"))
    return jax.shard_map(
        functools.partial(per_device, mesh.shape["grp"], mesh.shape["sub"]),
        mesh=mesh,
        in_specs=(both,) * 8,
        out_specs=(P("grp", "sub", None), both),
        check_vma=False,
    )
```
